32 devices in a mesh: ep: 8 (over z, y), tp: 4 (over x, core).
Axes of the slice: x: 2, y: 2, z: 4, core: 2. Of those that a mesh axis runs over, the one named last changes fastest.
Arguments:
- tokens: bfloat16 [512, 4096], P(('ep', 'tp')), may hold values from -6 to 6
- routes: int32 [512, 2], P(('ep', 'tp')), may hold values from 0 to 7, all different within a row; in each aligned block of 16 rows (0 to 15, 16 to 31, ...) at most 8 rows name the same one
- combine: float32 [512, 2], P(('ep', 'tp')), may hold values from 0.25 to 1
- gate_weight: bfloat16 [8, 4096, 4096], P('ep', None, 'tp'), may hold values from -0.09375 to 0.09375
- up_weight: bfloat16 [8, 4096, 4096], P('ep', None, 'tp'), may hold values from -0.09375 to 0.09375
- down_weight: bfloat16 [8, 4096, 4096], P('ep', 'tp'), may hold values from -0.09375 to 0.09375
Outputs:
- moe_output: bfloat16 [512, 4096], P(('ep', 'tp'))
The draws below stay inside these ranges and needn't reach their ends.
Inputs may be any that keep to these rules, and one draw needn't show every extreme that they name: `routes`: each row names 2 different experts. Among the rows of one device no expert is named more than 8 times, and in every draw some expert is named exactly 8 times by the rows of some device.
All inputs are finite; a program needn't handle non-finite values.
Results may differ from the reference program's by a relative error of at most 0.015.
Values may be sent and summed in bfloat16 or wider, within the bound.
A program may use at most 64 MiB of HBM per device.

```python
import math
import jax
import jax.numpy as jnp
import numpy as np
from jax import lax

D = 4096
FF = 4096
TOP = 2
TOK_DEV = 16
E = 8
FF_DEV = 1024
C = 8
TOKENS = 512
N_TP = 4
DEVICES = 32


def block_scale(rng, dims, split, smallest, top_value):
    def one(dim, parts):
        steps = jax.random.uniform(jax.random.fold_in(jax.random.fold_in(rng, 6), dim), (parts,), jnp.float32, smallest / len(split), top_value / len(split))
        return jnp.repeat(jnp.exp(steps), dims[dim] // parts).reshape((-1,) + (1,) * (len(dims) - dim - 1))

    gain = one(*split[0])
    for cut in split[1:]:
        gain = gain * one(*cut)
    return gain


def assign_block(stream_key, own, number, rows, number_of, top, bound, slope):
    ranking = jax.random.permutation(stream_key, number_of)
    crowded, common = shares(number_of, rows * top, bound, slope, True), shares(number_of, rows * top, bound, slope, False)
    places = jnp.arange(number_of)

    def named(sizes, offset_by):
        used = int((sizes > 0).sum())
        fixed = max(1, used // 4)
        shifted = fixed + (places - fixed + offset_by * (used - fixed)) % max(1, number_of - fixed)
        return jnp.zeros((number_of,), jnp.int32).at[ranking[jnp.where(places < fixed, places, shifted)]].set(jnp.asarray(sizes, jnp.int32))

    sizes = jnp.where(number % 4 == 0, named(crowded, number // 4), named(common, number - number // 4 - 1))
    mixed = jax.random.permutation(jax.random.fold_in(own, 3), number_of)
    giver, sink = mixed[0:number_of // 2 * 2:2], mixed[1:number_of // 2 * 2:2]
    slack = jnp.minimum(sizes[giver] - 1, bound - sizes[sink]) // 2
    slack = jnp.where((giver == ranking[0]) | (sink == ranking[0]) | (sizes[sink] == 0), 0, jnp.maximum(slack, 0))
    shifted = jax.random.randint(jax.random.fold_in(own, 4), (number_of // 2,), 0, 1 << 20) % (slack + 1)
    sizes = sizes.at[giver].add(-shifted).at[sink].add(shifted)
    items = jnp.searchsorted(jnp.cumsum(sizes), jnp.arange(rows * top), side="right").astype(jnp.int32)
    table = items.reshape(top, rows).T
    table = table[jax.random.permutation(jax.random.fold_in(own, 1), rows)]
    offset_by = jax.random.randint(jax.random.fold_in(own, 2), (rows, 1), 0, top)
    return jnp.take_along_axis(table, (jnp.arange(top)[None, :] + offset_by) % top, axis=1)


def shares(number_of, total, bound, skew, full):
    loads = [(1 << 20) // math.isqrt(grade ** skew) + 1 for grade in range(1, number_of + 1)]
    largest = bound if full else min(bound, max(-(-total // number_of), total * loads[0] // sum(loads)))
    least = 1 if total - largest >= number_of - 1 else 0
    holding, surplus = [largest] + [least] * (number_of - 1), total - largest - least * (number_of - 1)
    while surplus > 0:
        candidates = [i for i in range(1, number_of) if holding[i] < largest] or [i for i in range(1, number_of) if holding[i] < bound]
        pool, remaining = sum([loads[i] for i in candidates]), surplus
        for i in candidates:
            addition = min(bound - holding[i], max(1, remaining * loads[i] // pool), surplus)
            holding[i] = holding[i] + addition
            surplus = surplus - addition
    return np.array(holding)


def centred(stream_key, shape, width, bound, split=(), kind=jnp.bfloat16):
    drawn = jax.random.normal(stream_key, shape, jnp.float32) * width
    if len(split) > 0:
        drawn = block_scale(stream_key, shape, split, -0.22, 0.18) * drawn
    return jnp.clip(drawn, min=-bound, max=bound).astype(kind)


def setup_inputs(seed: int = 0) -> dict:
    splits = jax.random.split(jax.random.key(seed), 7)
    tokens = centred(splits[0], (TOKENS, D), 1.0, 6.0, ((0, 32),))
    routes_keys = jax.random.split(jax.random.fold_in(splits[1], 1), TOKENS // TOK_DEV)
    routes_turns = jax.random.permutation(jax.random.fold_in(splits[1], 3), TOKENS // TOK_DEV)
    routes = jax.vmap(lambda own, number: assign_block(jax.random.fold_in(splits[1], 2), own, number, TOK_DEV, E, TOP, C, 2))(routes_keys, routes_turns).reshape((TOKENS, TOP))
    combine = jnp.clip(0.25 + 0.75 * jax.random.uniform(splits[2], (TOKENS, TOP), jnp.float32) ** block_scale(splits[2], (TOKENS, TOP), ((0, 32),), -0.2, 0.2), 0.25, 1.0)
    gate_weight = centred(splits[3], (E, D, FF), D ** -0.5, 0.09375, ((0, 8), (2, 4)))
    up_weight = centred(splits[4], (E, D, FF), D ** -0.5, 0.09375, ((0, 8), (2, 4)))
    down_weight = centred(splits[5], (E, FF, D), FF ** -0.5, 0.09375, ((0, 8), (1, 4)))
    return dict(tokens=tokens, routes=routes, combine=combine, gate_weight=gate_weight, up_weight=up_weight, down_weight=down_weight)


def reference(tokens, routes, combine, gate_weight, up_weight, down_weight):
    assignments = TOK_DEV * TOP
    flat_ids = routes.reshape(DEVICES, assignments).astype(jnp.int32)
    onehot = (flat_ids[:, :, None] == jnp.arange(E, dtype=jnp.int32)[None, None, :]).astype(jnp.int32)
    earlier = jnp.cumsum(onehot, axis=1) - onehot
    slot_index = jnp.sum(earlier * onehot, axis=2)
    target = flat_ids * C + slot_index
    selector = (target[:, :, None] == jnp.arange(E * C, dtype=jnp.int32)[None, None, :]).astype(jnp.float32)
    repeated = jnp.repeat(tokens.reshape(DEVICES, TOK_DEV, D), TOP, axis=1).astype(jnp.float32)
    buffer = jnp.einsum("sak,sad->skd", selector, repeated, precision=lax.Precision.HIGHEST).astype(jnp.bfloat16)
    buffer = buffer.reshape(DEVICES, E, C, D).transpose(1, 0, 2, 3).reshape(E, DEVICES * C, D)

    def expert(operands):
        inputs, w_gate, w_up, w_down = operands
        gate_values = jnp.dot(inputs, w_gate, preferred_element_type=jnp.float32)
        up_values = jnp.dot(inputs, w_up, preferred_element_type=jnp.float32)
        hidden = (jax.nn.silu(gate_values) * up_values).astype(jnp.bfloat16)
        hidden_split = hidden.reshape(DEVICES * C, N_TP, FF_DEV).astype(jnp.float32)
        down_split = w_down.reshape(N_TP, FF_DEV, D).astype(jnp.float32)
        group_parts = jnp.einsum("rgf,gfd->grd", hidden_split, down_split, precision=lax.Precision.HIGHEST).astype(jnp.bfloat16)
        return jnp.sum(group_parts.astype(jnp.float32), axis=0).astype(jnp.bfloat16)

    expert_results = lax.map(expert, (buffer, gate_weight, up_weight, down_weight))
    returned = expert_results.reshape(E, DEVICES, C, D).transpose(1, 0, 2, 3).reshape(DEVICES, E * C, D).astype(jnp.float32)
    picked = jnp.einsum("sak,skd->sad", selector, returned, precision=lax.Precision.HIGHEST).reshape(TOKENS, TOP, D)
    return jnp.sum(combine[:, :, None] * picked, axis=1).astype(jnp.bfloat16)
```

```python
import functools
import jax
import jax.numpy as jnp
from jax import lax
from jax.experimental import pallas as pl
from jax.experimental.pallas import tpu as pltpu
from jax.sharding import PartitionSpec as P

MESH = pl.DeviceIdType.MESH
F32, BF16 = jnp.float32, jnp.bfloat16


def kernel(
    tokens_ref, routes_ref, combine_ref, gate_hbm, up_hbm, down_hbm, out_ref,
    gate_ref, up_ref, down_ref, slots, rows, gate_acc, up_acc, hidden,
    part, pair, summed, across, ready, back, weights,
    w_sem, a_send, a_recv, x_send, x_recv, d_send, d_recv,
    q_send, q_recv, t_send, t_recv, v_send, v_recv,
    *, experts, capacity, pad,
):
    token_rows, width = tokens_ref.shape
    chunks, cut = rows.shape[0], rows.shape[-1]
    sides = rows.shape[2]
    inner = gate_ref.shape[-1]
    all_rows = 2 * sides * experts * pad
    me = lax.axis_index("ep")
    tp = lax.axis_index("tp")
    core = lax.rem(tp, 2)
    side = lax.div(tp, 2)
    mate = 1 - core

    def ep_peer(i):
        return lax.rem(me + i, experts)

    def side_peer(i):
        return lax.rem(side + i, sides)

    def at_ep(e):
        return {"ep": e, "tp": tp}

    def at_side(s):
        return {"ep": me, "tp": s * 2 + core}

    at_mate = {"ep": me, "tp": side * 2 + mate}

    def remote(src, dst, send, recv, target):
        return pltpu.make_async_remote_copy(
            src_ref=src, dst_ref=dst, send_sem=send, recv_sem=recv,
            device_id=target, device_id_type=MESH,
        )

    def weight_copies(k):
        span = pl.ds(pl.multiple_of(k * cut, cut), cut)
        return (
            pltpu.make_async_copy(gate_hbm.at[0, span, :], gate_ref.at[k], w_sem.at[0, k]),
            pltpu.make_async_copy(up_hbm.at[0, span, :], up_ref.at[k], w_sem.at[1, k]),
        )

    def down_copy(k):
        span = pl.ds(pl.multiple_of(k * cut, cut), cut)
        return pltpu.make_async_copy(down_hbm.at[0, :, span], down_ref.at[k], w_sem.at[2, k])

    barrier = pltpu.get_barrier_semaphore()
    for i in range(1, experts):
        pl.semaphore_signal(barrier, inc=1, device_id=at_ep(ep_peer(i)), device_id_type=MESH)
    for i in range(1, sides):
        pl.semaphore_signal(barrier, inc=1, device_id=at_side(side_peer(i)), device_id_type=MESH)
    pl.semaphore_signal(barrier, inc=1, device_id=at_mate, device_id_type=MESH)

    for k in range(chunks):
        for copy in weight_copies(k):
            copy.start()

    column = lax.broadcasted_iota(jnp.int32, (token_rows, experts * pad), 1)
    column_expert, column_slot = lax.div(column, pad), lax.rem(column, pad)
    first = routes_ref[:, 0:1] == column_expert
    second = routes_ref[:, 1:2] == column_expert
    named = jnp.where(first, 1.0, 0.0) + jnp.where(second, 1.0, 0.0)
    row_at = lax.broadcasted_iota(jnp.int32, (token_rows, token_rows), 0)
    row_of = lax.broadcasted_iota(jnp.int32, (token_rows, token_rows), 1)
    before = jnp.where(row_of < row_at, 1.0, 0.0)
    earlier = jnp.dot(before.astype(BF16), named.astype(BF16), preferred_element_type=F32)
    taken = earlier == column_slot.astype(F32)
    selector = jnp.where(taken, named, 0.0).astype(BF16)
    share = jnp.where(first, combine_ref[:, 0:1], 0.0) + jnp.where(second, combine_ref[:, 1:2], 0.0)
    share = jnp.where(taken, share, 0.0)
    share_high = share.astype(BF16)
    weights[0:token_rows, :] = share_high.astype(F32)
    weights[token_rows : 2 * token_rows, :] = share - share_high.astype(F32)

    pl.semaphore_wait(barrier, experts - 1 + sides)

    def a_copy(k, e):
        return remote(
            slots.at[k, e], rows.at[k, core, side, me], a_send.at[k, e], a_recv.at[k, me], at_ep(e)
        )

    for k in range(chunks):
        block = lax.dot_general(
            selector, tokens_ref[:, k * cut : (k + 1) * cut],
            (((0,), (0,)), ((), ())), preferred_element_type=F32,
        )
        slots[k] = block.reshape(experts, pad, cut).astype(BF16)
        for i in range(1, experts):
            a_copy(k, ep_peer(i)).start()
        rows[k, core, side, me] = slots[k, me]
    for k in range(chunks):
        down_copy(k).start()

    def x_copy(k, s):
        return remote(
            rows.at[k, core, side], rows.at[k, core, side],
            x_send.at[k, s], x_recv.at[k, side], at_side(s),
        )

    def d_copy(k, s):
        return remote(
            rows.at[k, core, s], rows.at[k, core, s], d_send.at[k, s], d_recv.at[k, s], at_mate
        )

    gate_acc[...] = jnp.zeros_like(gate_acc)
    up_acc[...] = jnp.zeros_like(up_acc)

    def dispatch(step, carry):
        @pl.when(step < chunks)
        def _():
            k = step
            for i in range(1, experts):
                e = ep_peer(i)
                remote(
                    slots.at[k, e], rows.at[k, core, side, e],
                    a_send.at[k, e], a_recv.at[k, e], at_ep(e),
                ).wait_recv()
            for i in range(1, sides):
                x_copy(k, side_peer(i)).start()
            d_copy(k, side).start()

        @pl.when(jnp.logical_and(step >= 1, step < chunks + 1))
        def _():
            k = step - 1
            for i in range(1, sides):
                s = side_peer(i)
                remote(
                    rows.at[k, core, s], rows.at[k, core, s],
                    x_send.at[k, s], x_recv.at[k, s], at_side(s),
                ).wait_recv()
                d_copy(k, s).start()

        @pl.when(step >= 2)
        def _():
            k = step - 2
            for copy in weight_copies(k):
                copy.wait()
            for s in range(sides):
                remote(
                    rows.at[k, mate, s], rows.at[k, mate, s],
                    d_send.at[k, s], d_recv.at[k, s], at_mate,
                ).wait_recv()
            x = rows[k].astype(F32).reshape(all_rows, cut).astype(BF16)
            gate_acc[...] += jnp.dot(x, gate_ref[k], preferred_element_type=F32)
            up_acc[...] += jnp.dot(x, up_ref[k], preferred_element_type=F32)

        return carry

    lax.fori_loop(0, chunks + 2, dispatch, 0)

    gates = gate_acc[...]
    hidden[...] = (gates / (1.0 + jnp.exp(-gates)) * up_acc[...]).astype(BF16)

    def q_copy(k):
        return remote(part.at[k, mate], pair.at[k], q_send.at[k], q_recv.at[k], at_mate)

    def t_copy(k, s):
        return remote(
            summed.at[k, s], across.at[k, side], t_send.at[k, s], t_recv.at[k, side], at_side(s)
        )

    def v_copy(k, e):
        return remote(ready.at[k, e], back.at[k, me], v_send.at[k, e], v_recv.at[k, me], at_ep(e))

    def down(step, carry):
        @pl.when(step < chunks)
        def _():
            k = step
            down_copy(k).wait()
            block = jnp.dot(hidden[...], down_ref[k], preferred_element_type=F32)
            part[k] = block.reshape(2, sides, experts, pad, cut).astype(BF16)
            q_copy(k).start()

        @pl.when(step >= 2)
        def _():
            k = step - 2
            q_copy(k).wait_recv()
            for i in range(1, sides):
                s = side_peer(i)
                summed[k, s] = (part[k, core, s].astype(F32) + pair[k, s].astype(F32)).astype(BF16)
                t_copy(k, s).start()

        return carry

    lax.fori_loop(0, chunks + 2, down, 0)

    share_rows = weights[...].astype(BF16)

    def finish(step, carry):
        @pl.when(step < chunks)
        def _():
            k = step
            total = part[k, core, side].astype(F32) + pair[k, side].astype(F32)
            for i in range(1, sides):
                s = side_peer(i)
                remote(
                    summed.at[k, s], across.at[k, s],
                    t_send.at[k, s], t_recv.at[k, s], at_side(s),
                ).wait_recv()
                total = total + across[k, s].astype(F32)
            ready[k] = total.astype(BF16)
            for i in range(1, experts):
                v_copy(k, ep_peer(i)).start()
            back[k, me] = ready[k, me]

        @pl.when(step >= 1)
        def _():
            k = step - 1
            for i in range(1, experts):
                e = ep_peer(i)
                remote(
                    ready.at[k, e], back.at[k, e], v_send.at[k, e], v_recv.at[k, e], at_ep(e)
                ).wait_recv()
            returned = back[k].astype(F32).reshape(experts * pad, cut).astype(BF16)
            both = jnp.dot(share_rows, returned, preferred_element_type=F32)
            span = pl.ds(pl.multiple_of(k * cut, cut), cut)
            out_ref[:, span] = (both[:token_rows] + both[token_rows:]).astype(BF16)

        return carry

    lax.fori_loop(0, chunks + 1, finish, 0)

    def drain(k, carry):
        for i in range(1, experts):
            a_copy(k, ep_peer(i)).wait_send()
            v_copy(k, ep_peer(i)).wait_send()
        for i in range(1, sides):
            x_copy(k, side_peer(i)).wait_send()
            t_copy(k, side_peer(i)).wait_send()
        for s in range(sides):
            d_copy(k, s).wait_send()
        q_copy(k).wait_send()
        return carry

    lax.fori_loop(0, chunks, drain, 0)


def body(tokens, routes, combine, gate_weight, up_weight, down_weight):
    token_rows, width = tokens.shape
    top = routes.shape[1]
    inner = gate_weight.shape[-1]
    experts = lax.axis_size("ep")
    sides = lax.axis_size("tp") // 2
    capacity = 2 * token_rows * top // experts
    pad = -(-capacity // 8) * 8
    cut = min(512, width)
    chunks = width // cut
    all_rows = 2 * sides * experts * pad
    vmem, dma = pltpu.VMEM, pltpu.SemaphoreType.DMA
    in_vmem = pl.BlockSpec(memory_space=pltpu.VMEM)
    in_hbm = pl.BlockSpec(memory_space=pl.ANY)
    group = (experts, pad, cut)
    return pl.pallas_call(
        functools.partial(kernel, experts=experts, capacity=capacity, pad=pad),
        out_shape=jax.ShapeDtypeStruct((token_rows, width), BF16),
        in_specs=[in_vmem] * 3 + [in_hbm] * 3,
        out_specs=in_vmem,
        scratch_shapes=[
            vmem((chunks, cut, inner), BF16),
            vmem((chunks, cut, inner), BF16),
            vmem((chunks, inner, cut), BF16),
            vmem((chunks,) + group, BF16),
            vmem((chunks, 2, sides) + group, BF16),
            vmem((all_rows, inner), F32),
            vmem((all_rows, inner), F32),
            vmem((all_rows, inner), BF16),
            vmem((chunks, 2, sides) + group, BF16),
            vmem((chunks, sides) + group, BF16),
            vmem((chunks, sides) + group, BF16),
            vmem((chunks, sides) + group, BF16),
            vmem((chunks,) + group, BF16),
            vmem((chunks,) + group, BF16),
            vmem((2 * token_rows, experts * pad), F32),
            dma((3, chunks)),
            dma((chunks, experts)), dma((chunks, experts)),
            dma((chunks, sides)), dma((chunks, sides)),
            dma((chunks, sides)), dma((chunks, sides)),
            dma((chunks,)), dma((chunks,)),
            dma((chunks, sides)), dma((chunks, sides)),
            dma((chunks, experts)), dma((chunks, experts)),
        ],
        compiler_params=pltpu.CompilerParams(
            collective_id=0, has_side_effects=True, vmem_limit_bytes=60 * 1024 * 1024
        ),
    )(tokens, routes, combine, gate_weight, up_weight, down_weight)


def solution(mesh):
    return jax.shard_map(
        body,
        mesh=mesh,
        in_specs=(
            P(("ep", "tp"), None),
            P(("ep", "tp"), None),
            P(("ep", "tp"), None),
            P("ep", None, "tp"),
            P("ep", None, "tp"),
            P("ep", "tp", None),
        ),
        out_specs=P(("ep", "tp"), None),
        check_vma=False,
    )
```

```python
import functools
import jax
import jax.numpy as jnp
from jax import lax
from jax.experimental import pallas as pl
from jax.experimental.pallas import tpu as pltpu
from jax.sharding import PartitionSpec as P

MESH = pl.DeviceIdType.MESH
F32, BF16 = jnp.float32, jnp.bfloat16


def kernel(
    tokens_ref, routes_ref, combine_ref, gate_hbm, up_hbm, down_hbm, out_ref,
    gate_ref, up_ref, down_ref, slots, rows, gate_acc, up_acc, hidden,
    part, pair, summed, across, ready, back, weights,
    w_sem, a_send, a_recv, x_send, x_recv, d_send, d_recv,
    q_send, q_recv, t_send, t_recv, v_send, v_recv,
    *, experts, capacity, pad,
):
    token_rows, width = tokens_ref.shape
    chunks, cut = rows.shape[0], rows.shape[-1]
    sides = rows.shape[2]
    inner = gate_ref.shape[-1]
    all_rows = 2 * sides * experts * pad
    me = lax.axis_index("ep")
    tp = lax.axis_index("tp")
    core = lax.rem(tp, 2)
    side = lax.div(tp, 2)
    mate = 1 - core

    lanes = 2 if experts % 2 == 0 else 1
    lines = experts // lanes
    line, lane = lax.div(me, lanes), lax.rem(me, lanes)
    far = sorted(range(1, lines), key=lambda d: (-min(d, lines - d), d)) + [0]
    near = far[::-1]

    def line_peer(d):
        return lax.rem(line + d, lines)

    def ep_at(d, b):
        return line_peer(d) * lanes + lax.rem(lane + b, lanes)

    ep_peers = [(d, b) for d in far for b in range(lanes) if (d, b) != (0, 0)]

    def ep_peer(i):
        return ep_at(*ep_peers[i - 1])

    def side_peer(i):
        return lax.rem(side + i, sides)

    def at_ep(e):
        return {"ep": e, "tp": tp}

    def at_side(s):
        return {"ep": me, "tp": s * 2 + core}

    at_mate = {"ep": me, "tp": side * 2 + mate}

    def remote(src, dst, send, recv, target):
        return pltpu.make_async_remote_copy(
            src_ref=src, dst_ref=dst, send_sem=send, recv_sem=recv,
            device_id=target, device_id_type=MESH,
        )

    def weight_copies(k):
        span = pl.ds(pl.multiple_of(k * cut, cut), cut)
        return (
            pltpu.make_async_copy(gate_hbm.at[0, span, :], gate_ref.at[k], w_sem.at[0, k]),
            pltpu.make_async_copy(up_hbm.at[0, span, :], up_ref.at[k], w_sem.at[1, k]),
        )

    def down_copy(k):
        span = pl.ds(pl.multiple_of(k * cut, cut), cut)
        return pltpu.make_async_copy(down_hbm.at[0, :, span], down_ref.at[k], w_sem.at[2, k])

    barrier = pltpu.get_barrier_semaphore()
    for i in range(1, experts):
        pl.semaphore_signal(barrier, inc=1, device_id=at_ep(ep_peer(i)), device_id_type=MESH)
    for i in range(1, sides):
        pl.semaphore_signal(barrier, inc=1, device_id=at_side(side_peer(i)), device_id_type=MESH)
    pl.semaphore_signal(barrier, inc=1, device_id=at_mate, device_id_type=MESH)

    for k in range(chunks):
        for copy in weight_copies(k):
            copy.start()

    place = lax.broadcasted_iota(jnp.int32, (experts * pad, token_rows), 0)
    place_expert, place_slot = lax.div(place, pad), lax.rem(place, pad)
    first = routes_ref[0:1, :] == place_expert
    second = routes_ref[1:2, :] == place_expert
    named = jnp.where(first, 1.0, 0.0) + jnp.where(second, 1.0, 0.0)
    row_of = lax.broadcasted_iota(jnp.int32, (token_rows, token_rows), 0)
    row_at = lax.broadcasted_iota(jnp.int32, (token_rows, token_rows), 1)
    before = jnp.where(row_of < row_at, 1.0, 0.0)
    earlier = jnp.dot(named.astype(BF16), before.astype(BF16), preferred_element_type=F32)
    taken = earlier == place_slot.astype(F32)
    selector = jnp.where(taken, named, 0.0).astype(BF16)
    share = jnp.where(first, combine_ref[0:1, :], 0.0) + jnp.where(second, combine_ref[1:2, :], 0.0)
    share = jnp.where(taken, share, 0.0)
    share_high = share.astype(BF16).astype(F32)
    weights[:, 0:token_rows] = share_high
    weights[:, token_rows : 2 * token_rows] = share - share_high

    pl.semaphore_wait(barrier, experts - 1 + sides)

    def a_copy(k, e):
        return remote(
            slots.at[k, e], rows.at[k, core, side, me], a_send.at[k, e], a_recv.at[k, me], at_ep(e)
        )

    for k in range(chunks):
        block = lax.dot_general(
            selector, tokens_ref[:, k * cut : (k + 1) * cut],
            (((1,), (0,)), ((), ())), preferred_element_type=F32,
        )
        slots[k] = block.reshape(experts, pad, cut).astype(BF16)
        for i in range(1, experts):
            a_copy(k, ep_peer(i)).start()
        rows[k, core, side, me] = slots[k, me]
    for k in range(chunks):
        down_copy(k).start()

    def row_block(k, c, s, z):
        return rows.at[k, c, s, pl.ds(z * lanes, lanes)]

    def x_copy(k, s, z):
        block = row_block(k, core, side, z)
        return remote(block, block, x_send.at[k, s, z], x_recv.at[k, side, z], at_side(s))

    def x_arrival(k, s, z):
        block = row_block(k, core, s, z)
        return remote(block, block, x_send.at[k, s, z], x_recv.at[k, s, z], at_side(s))

    def d_copy(k, s, z):
        block = row_block(k, core, s, z)
        return remote(block, block, d_send.at[k, s, z], d_recv.at[k, s, z], at_mate)

    def d_arrival(k, s, z):
        block = row_block(k, mate, s, z)
        return remote(block, block, d_send.at[k, s, z], d_recv.at[k, s, z], at_mate)

    gate_acc[...] = jnp.zeros_like(gate_acc)
    up_acc[...] = jnp.zeros_like(up_acc)

    def dispatch(step, carry):
        @pl.when(step < chunks)
        def _():
            k = step
            for d in near:
                z = line_peer(d)
                for b in range(lanes):
                    if (d, b) != (0, 0):
                        e = ep_at(d, b)
                        remote(
                            slots.at[k, e], rows.at[k, core, side, e],
                            a_send.at[k, e], a_recv.at[k, e], at_ep(e),
                        ).wait_recv()
                for i in range(1, sides):
                    x_copy(k, side_peer(i), z).start()
                d_copy(k, side, z).start()

        @pl.when(jnp.logical_and(step >= 1, step < chunks + 1))
        def _():
            k = step - 1
            for d in near:
                z = line_peer(d)
                for i in range(1, sides):
                    s = side_peer(i)
                    x_arrival(k, s, z).wait_recv()
                    d_copy(k, s, z).start()

        @pl.when(step >= 2)
        def _():
            k = step - 2
            for copy in weight_copies(k):
                copy.wait()
            for s in range(sides):
                for z in range(lines):
                    d_arrival(k, s, z).wait_recv()
            x = rows[k].astype(F32).reshape(all_rows, cut).astype(BF16)
            gate_acc[...] += jnp.dot(x, gate_ref[k], preferred_element_type=F32)
            up_acc[...] += jnp.dot(x, up_ref[k], preferred_element_type=F32)

        return carry

    lax.fori_loop(0, chunks + 2, dispatch, 0)

    gates = gate_acc[...]
    hidden[...] = (gates / (1.0 + jnp.exp(-gates)) * up_acc[...]).astype(BF16)

    def q_copy(k):
        return remote(part.at[k, mate], pair.at[k], q_send.at[k], q_recv.at[k], at_mate)

    def t_copy(k, s, z):
        span = pl.ds(z * lanes, lanes)
        return remote(
            summed.at[k, s, span], across.at[k, side, span],
            t_send.at[k, s, z], t_recv.at[k, side, z], at_side(s),
        )

    def t_arrival(k, s, z):
        span = pl.ds(z * lanes, lanes)
        return remote(
            summed.at[k, s, span], across.at[k, s, span],
            t_send.at[k, s, z], t_recv.at[k, s, z], at_side(s),
        )

    def v_copy(k, e):
        return remote(ready.at[k, e], back.at[k, me], v_send.at[k, e], v_recv.at[k, me], at_ep(e))

    def down(step, carry):
        @pl.when(step < chunks)
        def _():
            k = step
            down_copy(k).wait()
            block = jnp.dot(hidden[...], down_ref[k], preferred_element_type=F32)
            part[k] = block.reshape(2, sides, experts, pad, cut).astype(BF16)
            q_copy(k).start()

        @pl.when(step >= 2)
        def _():
            k = step - 2
            q_copy(k).wait_recv()
            for i in range(1, sides):
                s = side_peer(i)
                summed[k, s] = (part[k, core, s].astype(F32) + pair[k, s].astype(F32)).astype(BF16)
                for d in far:
                    t_copy(k, s, line_peer(d)).start()

        return carry

    lax.fori_loop(0, chunks + 2, down, 0)

    share_rows = jnp.transpose(weights[...]).astype(BF16)

    def finish(step, carry):
        @pl.when(step < chunks)
        def _():
            k = step
            for d in far:
                z = line_peer(d)
                span = pl.ds(z * lanes, lanes)
                total = part[k, core, side, span].astype(F32) + pair[k, side, span].astype(F32)
                for i in range(1, sides):
                    s = side_peer(i)
                    t_arrival(k, s, z).wait_recv()
                    total = total + across[k, s, span].astype(F32)
                ready[k, span] = total.astype(BF16)
                for b in range(lanes):
                    if (d, b) != (0, 0):
                        v_copy(k, ep_at(d, b)).start()
            back[k, me] = ready[k, me]

        @pl.when(step >= 1)
        def _():
            k = step - 1
            for i in range(1, experts):
                e = ep_peer(i)
                remote(
                    ready.at[k, e], back.at[k, e], v_send.at[k, e], v_recv.at[k, e], at_ep(e)
                ).wait_recv()
            returned = back[k].astype(F32).reshape(experts * pad, cut).astype(BF16)
            both = jnp.dot(share_rows, returned, preferred_element_type=F32)
            span = pl.ds(pl.multiple_of(k * cut, cut), cut)
            out_ref[:, span] = (both[:token_rows] + both[token_rows:]).astype(BF16)

        return carry

    lax.fori_loop(0, chunks + 1, finish, 0)

    def drain(k, carry):
        for i in range(1, experts):
            a_copy(k, ep_peer(i)).wait_send()
            v_copy(k, ep_peer(i)).wait_send()
        for z in range(lines):
            for i in range(1, sides):
                x_copy(k, side_peer(i), z).wait_send()
                t_copy(k, side_peer(i), z).wait_send()
            for s in range(sides):
                d_copy(k, s, z).wait_send()
        q_copy(k).wait_send()
        return carry

    lax.fori_loop(0, chunks, drain, 0)


def body(tokens, routes, combine, gate_weight, up_weight, down_weight):
    token_rows, width = tokens.shape
    top = routes.shape[1]
    inner = gate_weight.shape[-1]
    experts = lax.axis_size("ep")
    sides = lax.axis_size("tp") // 2
    capacity = 2 * token_rows * top // experts
    pad = -(-capacity // 8) * 8
    cut = min(1024, width)
    chunks = width // cut
    lines = experts // 2 if experts % 2 == 0 else experts
    all_rows = 2 * sides * experts * pad
    vmem, dma = pltpu.VMEM, pltpu.SemaphoreType.DMA
    in_vmem = pl.BlockSpec(memory_space=pltpu.VMEM)
    in_hbm = pl.BlockSpec(memory_space=pl.ANY)
    group = (experts, pad, cut)
    return pl.pallas_call(
        functools.partial(kernel, experts=experts, capacity=capacity, pad=pad),
        out_shape=jax.ShapeDtypeStruct((token_rows, width), BF16),
        in_specs=[in_vmem] * 3 + [in_hbm] * 3,
        out_specs=in_vmem,
        scratch_shapes=[
            vmem((chunks, cut, inner), BF16),
            vmem((chunks, cut, inner), BF16),
            vmem((chunks, inner, cut), BF16),
            vmem((chunks,) + group, BF16),
            vmem((chunks, 2, sides) + group, BF16),
            vmem((all_rows, inner), F32),
            vmem((all_rows, inner), F32),
            vmem((all_rows, inner), BF16),
            vmem((chunks, 2, sides) + group, BF16),
            vmem((chunks, sides) + group, BF16),
            vmem((chunks, sides) + group, BF16),
            vmem((chunks, sides) + group, BF16),
            vmem((chunks,) + group, BF16),
            vmem((chunks,) + group, BF16),
            vmem((experts * pad, 2 * token_rows), F32),
            dma((3, chunks)),
            dma((chunks, experts)), dma((chunks, experts)),
            dma((chunks, sides, lines)), dma((chunks, sides, lines)),
            dma((chunks, sides, lines)), dma((chunks, sides, lines)),
            dma((chunks,)), dma((chunks,)),
            dma((chunks, sides, lines)), dma((chunks, sides, lines)),
            dma((chunks, experts)), dma((chunks, experts)),
        ],
        compiler_params=pltpu.CompilerParams(
            collective_id=0, has_side_effects=True, vmem_limit_bytes=60 * 1024 * 1024
        ),
    )(tokens, routes.T, combine.T, gate_weight, up_weight, down_weight)


def solution(mesh):
    return jax.shard_map(
        body,
        mesh=mesh,
        in_specs=(
            P(("ep", "tp"), None),
            P(("ep", "tp"), None),
            P(("ep", "tp"), None),
            P("ep", None, "tp"),
            P("ep", None, "tp"),
            P("ep", "tp", None),
        ),
        out_specs=P(("ep", "tp"), None),
        check_vma=False,
    )
```

```python
import functools
import jax
import jax.numpy as jnp
from jax import lax
from jax.experimental import pallas as pl
from jax.experimental.pallas import tpu as pltpu
from jax.sharding import PartitionSpec as P

MESH = pl.DeviceIdType.MESH
F32, BF16 = jnp.float32, jnp.bfloat16


def kernel(
    tokens_ref, routes_ref, combine_ref, gate_hbm, up_hbm, down_hbm, out_ref,
    gate_ref, up_ref, down_ref, slots, rows, gate_acc, up_acc, hidden,
    part, pair, summed, across, ready, back, weights,
    w_sem, a_send, a_recv, x_send, x_recv, d_send, d_recv,
    q_send, q_recv, t_send, t_recv, v_send, v_recv,
    *, experts, capacity, pad,
):
    token_rows, width = tokens_ref.shape
    chunks, cut = rows.shape[0], rows.shape[-1]
    sides = rows.shape[2]
    inner = gate_ref.shape[-1]
    all_rows = 2 * sides * experts * pad
    me = lax.axis_index("ep")
    tp = lax.axis_index("tp")
    core = lax.rem(tp, 2)
    side = lax.div(tp, 2)
    mate = 1 - core

    lanes = 2 if experts % 2 == 0 else 1
    lines = experts // lanes
    line, lane = lax.div(me, lanes), lax.rem(me, lanes)
    far = sorted(range(1, lines), key=lambda d: (-min(d, lines - d), d)) + [0]
    near = far[::-1]

    def line_peer(d):
        return lax.rem(line + d, lines)

    def ep_at(d, b):
        return line_peer(d) * lanes + lax.rem(lane + b, lanes)

    ep_peers = [(d, b) for d in far for b in range(lanes) if (d, b) != (0, 0)]

    def ep_peer(i):
        return ep_at(*ep_peers[i - 1])

    def side_peer(i):
        return lax.rem(side + i, sides)

    def at_ep(e):
        return {"ep": e, "tp": tp}

    def at_side(s):
        return {"ep": me, "tp": s * 2 + core}

    at_mate = {"ep": me, "tp": side * 2 + mate}

    def remote(src, dst, send, recv, target):
        return pltpu.make_async_remote_copy(
            src_ref=src, dst_ref=dst, send_sem=send, recv_sem=recv,
            device_id=target, device_id_type=MESH,
        )

    def weight_copies(k):
        span = pl.ds(pl.multiple_of(k * cut, cut), cut)
        return (
            pltpu.make_async_copy(gate_hbm.at[0, span, :], gate_ref.at[k], w_sem.at[0, k]),
            pltpu.make_async_copy(up_hbm.at[0, span, :], up_ref.at[k], w_sem.at[1, k]),
        )

    def down_copy(k):
        span = pl.ds(pl.multiple_of(k * cut, cut), cut)
        return pltpu.make_async_copy(down_hbm.at[0, :, span], down_ref.at[k], w_sem.at[2, k])

    barrier = pltpu.get_barrier_semaphore()
    for i in range(1, experts):
        pl.semaphore_signal(barrier, inc=1, device_id=at_ep(ep_peer(i)), device_id_type=MESH)
    for i in range(1, sides):
        pl.semaphore_signal(barrier, inc=1, device_id=at_side(side_peer(i)), device_id_type=MESH)
    pl.semaphore_signal(barrier, inc=1, device_id=at_mate, device_id_type=MESH)

    for k in range(chunks):
        for copy in weight_copies(k):
            copy.start()

    place = lax.broadcasted_iota(jnp.int32, (experts * pad, token_rows), 0)
    place_expert, place_slot = lax.div(place, pad), lax.rem(place, pad)
    first = routes_ref[0:1, :] == place_expert
    second = routes_ref[1:2, :] == place_expert
    named = jnp.where(first, 1.0, 0.0) + jnp.where(second, 1.0, 0.0)
    row_of = lax.broadcasted_iota(jnp.int32, (token_rows, token_rows), 0)
    row_at = lax.broadcasted_iota(jnp.int32, (token_rows, token_rows), 1)
    before = jnp.where(row_of < row_at, 1.0, 0.0)
    earlier = jnp.dot(named.astype(BF16), before.astype(BF16), preferred_element_type=F32)
    taken = earlier == place_slot.astype(F32)
    selector = jnp.where(taken, named, 0.0).astype(BF16)
    share = jnp.where(first, combine_ref[0:1, :], 0.0) + jnp.where(second, combine_ref[1:2, :], 0.0)
    share = jnp.where(taken, share, 0.0)
    share_high = share.astype(BF16).astype(F32)
    weights[:, 0:token_rows] = share_high
    weights[:, token_rows : 2 * token_rows] = share - share_high

    pl.semaphore_wait(barrier, experts - 1 + sides)

    def a_copy(k, e):
        return remote(
            slots.at[k, e], rows.at[k, core, side, me], a_send.at[k, e], a_recv.at[k, me], at_ep(e)
        )

    for k in range(chunks):
        block = lax.dot_general(
            selector, tokens_ref[:, k * cut : (k + 1) * cut],
            (((1,), (0,)), ((), ())), preferred_element_type=F32,
        )
        slots[k] = block.reshape(experts, pad, cut).astype(BF16)
        for i in range(1, experts):
            a_copy(k, ep_peer(i)).start()
        rows[k, core, side, me] = slots[k, me]
    for k in range(chunks):
        down_copy(k).start()

    def row_block(k, c, s, z):
        return rows.at[k, c, s, pl.ds(z * lanes, lanes)]

    def x_copy(k, s, z):
        block = row_block(k, core, side, z)
        return remote(block, block, x_send.at[k, s, z], x_recv.at[k, side, z], at_side(s))

    def x_arrival(k, s, z):
        block = row_block(k, core, s, z)
        return remote(block, block, x_send.at[k, s, z], x_recv.at[k, s, z], at_side(s))

    def d_copy(k, s, z):
        block = rows.at[k, core, s]
        return remote(block, block, d_send.at[k, s, z], d_recv.at[k, s, z], at_mate)

    def d_arrival(k, s, z):
        block = rows.at[k, mate, s]
        return remote(block, block, d_send.at[k, s, z], d_recv.at[k, s, z], at_mate)

    gate_acc[...] = jnp.zeros_like(gate_acc)
    up_acc[...] = jnp.zeros_like(up_acc)

    def dispatch(step, carry):
        @pl.when(step < chunks)
        def _():
            k = step
            for d in near:
                z = line_peer(d)
                for b in range(lanes):
                    if (d, b) != (0, 0):
                        e = ep_at(d, b)
                        remote(
                            slots.at[k, e], rows.at[k, core, side, e],
                            a_send.at[k, e], a_recv.at[k, e], at_ep(e),
                        ).wait_recv()
                for i in range(1, sides):
                    x_copy(k, side_peer(i), z).start()
            d_copy(k, side, 0).start()

        @pl.when(jnp.logical_and(step >= 1, step < chunks + 1))
        def _():
            k = step - 1
            for d in near:
                z = line_peer(d)
                for i in range(1, sides):
                    s = side_peer(i)
                    x_arrival(k, s, z).wait_recv()
            for i in range(1, sides):
                d_copy(k, side_peer(i), 0).start()

        @pl.when(step >= 2)
        def _():
            k = step - 2
            for copy in weight_copies(k):
                copy.wait()
            for s in range(sides):
                d_arrival(k, s, 0).wait_recv()
            x = rows[k].astype(F32).reshape(all_rows, cut).astype(BF16)
            gate_acc[...] += jnp.dot(x, gate_ref[k], preferred_element_type=F32)
            up_acc[...] += jnp.dot(x, up_ref[k], preferred_element_type=F32)

        return carry

    lax.fori_loop(0, chunks + 2, dispatch, 0)

    gates = gate_acc[...]
    hidden[...] = (gates / (1.0 + jnp.exp(-gates)) * up_acc[...]).astype(BF16)

    def q_copy(k):
        return remote(part.at[k, mate], pair.at[k], q_send.at[k], q_recv.at[k], at_mate)

    def t_copy(k, s, z):
        span = pl.ds(z * lanes, lanes)
        return remote(
            summed.at[k, s, span], across.at[k, side, span],
            t_send.at[k, s, z], t_recv.at[k, side, z], at_side(s),
        )

    def t_arrival(k, s, z):
        span = pl.ds(z * lanes, lanes)
        return remote(
            summed.at[k, s, span], across.at[k, s, span],
            t_send.at[k, s, z], t_recv.at[k, s, z], at_side(s),
        )

    def v_copy(k, e):
        return remote(ready.at[k, e], back.at[k, me], v_send.at[k, e], v_recv.at[k, me], at_ep(e))

    def down(step, carry):
        @pl.when(step < chunks)
        def _():
            k = step
            down_copy(k).wait()
            block = jnp.dot(hidden[...], down_ref[k], preferred_element_type=F32)
            part[k] = block.reshape(2, sides, experts, pad, cut).astype(BF16)
            q_copy(k).start()

        @pl.when(step >= 1)
        def _():
            k = step - 1
            q_copy(k).wait_recv()
            for i in range(1, sides):
                s = side_peer(i)
                summed[k, s] = (part[k, core, s].astype(F32) + pair[k, s].astype(F32)).astype(BF16)
                for d in far:
                    t_copy(k, s, line_peer(d)).start()

        return carry

    lax.fori_loop(0, chunks + 1, down, 0)

    share_rows = jnp.transpose(weights[...]).astype(BF16)

    def finish(step, carry):
        @pl.when(step < chunks)
        def _():
            k = step
            for d in far:
                z = line_peer(d)
                span = pl.ds(z * lanes, lanes)
                total = part[k, core, side, span].astype(F32) + pair[k, side, span].astype(F32)
                for i in range(1, sides):
                    s = side_peer(i)
                    t_arrival(k, s, z).wait_recv()
                    total = total + across[k, s, span].astype(F32)
                ready[k, span] = total.astype(BF16)
                for b in range(lanes):
                    if (d, b) != (0, 0):
                        v_copy(k, ep_at(d, b)).start()
            back[k, me] = ready[k, me]

        @pl.when(step >= 1)
        def _():
            k = step - 1
            for i in range(1, experts):
                e = ep_peer(i)
                remote(
                    ready.at[k, e], back.at[k, e], v_send.at[k, e], v_recv.at[k, e], at_ep(e)
                ).wait_recv()
            returned = back[k].astype(F32).reshape(experts * pad, cut).astype(BF16)
            both = jnp.dot(share_rows, returned, preferred_element_type=F32)
            span = pl.ds(pl.multiple_of(k * cut, cut), cut)
            out_ref[:, span] = (both[:token_rows] + both[token_rows:]).astype(BF16)

        return carry

    lax.fori_loop(0, chunks + 1, finish, 0)

    def drain(k, carry):
        for i in range(1, experts):
            a_copy(k, ep_peer(i)).wait_send()
            v_copy(k, ep_peer(i)).wait_send()
        for z in range(lines):
            for i in range(1, sides):
                x_copy(k, side_peer(i), z).wait_send()
                t_copy(k, side_peer(i), z).wait_send()
        for s in range(sides):
            d_copy(k, s, 0).wait_send()
        q_copy(k).wait_send()
        return carry

    lax.fori_loop(0, chunks, drain, 0)


def body(tokens, routes, combine, gate_weight, up_weight, down_weight):
    token_rows, width = tokens.shape
    top = routes.shape[1]
    inner = gate_weight.shape[-1]
    experts = lax.axis_size("ep")
    sides = lax.axis_size("tp") // 2
    capacity = 2 * token_rows * top // experts
    pad = -(-capacity // 8) * 8
    cut = min(1024, width)
    chunks = width // cut
    lines = experts // 2 if experts % 2 == 0 else experts
    all_rows = 2 * sides * experts * pad
    vmem, dma = pltpu.VMEM, pltpu.SemaphoreType.DMA
    in_vmem = pl.BlockSpec(memory_space=pltpu.VMEM)
    in_hbm = pl.BlockSpec(memory_space=pl.ANY)
    group = (experts, pad, cut)
    return pl.pallas_call(
        functools.partial(kernel, experts=experts, capacity=capacity, pad=pad),
        out_shape=jax.ShapeDtypeStruct((token_rows, width), BF16),
        in_specs=[in_vmem] * 3 + [in_hbm] * 3,
        out_specs=in_vmem,
        scratch_shapes=[
            vmem((chunks, cut, inner), BF16),
            vmem((chunks, cut, inner), BF16),
            vmem((chunks, inner, cut), BF16),
            vmem((chunks,) + group, BF16),
            vmem((chunks, 2, sides) + group, BF16),
            vmem((all_rows, inner), F32),
            vmem((all_rows, inner), F32),
            vmem((all_rows, inner), BF16),
            vmem((chunks, 2, sides) + group, BF16),
            vmem((chunks, sides) + group, BF16),
            vmem((chunks, sides) + group, BF16),
            vmem((chunks, sides) + group, BF16),
            vmem((chunks,) + group, BF16),
            vmem((chunks,) + group, BF16),
            vmem((experts * pad, 2 * token_rows), F32),
            dma((3, chunks)),
            dma((chunks, experts)), dma((chunks, experts)),
            dma((chunks, sides, lines)), dma((chunks, sides, lines)),
            dma((chunks, sides, lines)), dma((chunks, sides, lines)),
            dma((chunks,)), dma((chunks,)),
            dma((chunks, sides, lines)), dma((chunks, sides, lines)),
            dma((chunks, experts)), dma((chunks, experts)),
        ],
        compiler_params=pltpu.CompilerParams(
            collective_id=0, has_side_effects=True, vmem_limit_bytes=60 * 1024 * 1024
        ),
    )(tokens, routes.T, combine.T, gate_weight, up_weight, down_weight)


def solution(mesh):
    return jax.shard_map(
        body,
        mesh=mesh,
        in_specs=(
            P(("ep", "tp"), None),
            P(("ep", "tp"), None),
            P(("ep", "tp"), None),
            P("ep", None, "tp"),
            P("ep", None, "tp"),
            P("ep", "tp", None),
        ),
        out_specs=P(("ep", "tp"), None),
        check_vma=False,
    )
```
